32 devices in a mesh: ctx: 8 (over y, x, core), head: 4 (over z).
Axes of the slice: x: 2, y: 2, z: 4, core: 2. Of those that a mesh axis runs over, the one named last changes fastest.
Arguments:
- tokens: bfloat16 [2, 2048, 2048], P(None, 'ctx'), may hold values from -6 to 6
- w_qkv: bfloat16 [2048, 4, 1536], P(None, 'head'), as said below
- w_rate: bfloat16 [2048, 4], P(None, 'head'), may hold values from -0.125 to 0.125
- w_out: bfloat16 [4, 512, 2048], P('head'), may hold values from -0.125 to 0.125
- fw_gain: float32 [4, 512], P('head'), may hold values from 0.25 to 1.75
- fast_first: float32 [4, 512, 512], P('head'), may hold values from -0.25 to 0.25
- fast_third: float32 [4, 512, 512], P('head'), may hold values from -0.25 to 0.25
- fast_second: float32 [4, 512, 512], P('head'), may hold values from -0.25 to 0.25
Outputs:
- mixed: bfloat16 [2, 2048, 2048], P(None, 'ctx', 'head')
- new_first: float32 [4, 512, 512], P('head')
- new_third: float32 [4, 512, 512], P('head')
- new_second: float32 [4, 512, 512], P('head')
The draws below stay inside these ranges and needn't reach their ends.
Inputs may be any that keep to these rules, and one draw needn't show every extreme that they name: `w_qkv`: A projection scaled by its fan-in 2048.
All inputs are finite; a program needn't handle non-finite values.
Results may differ from the reference program's by a relative error of at most 0.039.
Values may be sent and summed in bfloat16 or wider, within the bound.
A program may use at most 128 MiB of HBM per device.

```python
import jax
import jax.numpy as jnp
from jax import lax

D = 2048
HEADS = 4
DH = 512
FH = 512
TOK_DEV = 256
WINDOW = 2048
BLOCKS = 2
NS_STEPS = 5
BLOCK = 2048


def draw_tokens(key, part):
    base = jax.random.normal(jax.random.fold_in(key, 11), (BLOCKS, BLOCK, D), jnp.float32)
    base = jnp.clip(base, -6.0, 6.0)
    return base.astype(jnp.bfloat16)


def draw_w_qkv(key, part):
    base = jax.random.normal(jax.random.fold_in(key, 23), (D, HEADS, 3 * DH), jnp.float32)
    base = jnp.clip(base, -6.0, 6.0) * D ** (-0.5)
    return base.astype(jnp.bfloat16)


def level_of(key, shape, pieces, low, high):
    loudness, own = 1.0, jax.random.fold_in(key, 6)
    for axis_at, parts in pieces:
        steps = jnp.exp(jax.random.uniform(jax.random.fold_in(own, axis_at), (parts,), jnp.float32, low / len(pieces), high / len(pieces)))
        loudness = loudness * jnp.repeat(steps, shape[axis_at] // parts).reshape([-1 if axis == axis_at else 1 for axis in range(len(shape))])
    return loudness


def scatter_about(rng, shape, spread, bound, cuts=(), held_as=jnp.bfloat16):
    drawn = spread * jax.random.normal(rng, shape, jnp.float32)
    if cuts:
        drawn = drawn * level_of(rng, shape, cuts, -0.22, 0.18)
    return jnp.clip(drawn, -bound, bound).astype(held_as)


def setup_inputs(seed: int = 0) -> dict:
    key_list = jax.random.split(jax.random.key(seed), 9)
    tokens = draw_tokens(jax.random.fold_in(key_list[8], 71), 0)
    w_qkv = draw_w_qkv(jax.random.fold_in(key_list[8], 71), 0)
    w_rate = scatter_about(key_list[2], (D, HEADS), D ** -0.5, 0.125, ((1, 4),))
    w_out = scatter_about(key_list[3], (HEADS, DH, D), D ** -0.5, 0.125, ((0, 4),))
    fw_gain = jnp.clip(1.0 + 0.15 * jax.random.normal(key_list[4], (HEADS, DH), jnp.float32), 0.25, 1.75)
    fast_first = scatter_about(key_list[5], (HEADS, DH, FH), DH ** -0.5, 0.25, ((0, 4),), jnp.float32)
    fast_third = scatter_about(key_list[6], (HEADS, DH, FH), DH ** -0.5, 0.25, ((0, 4),), jnp.float32)
    fast_second = scatter_about(key_list[7], (HEADS, FH, DH), FH ** -0.5, 0.25, ((0, 4),), jnp.float32)
    return dict(tokens=tokens, w_qkv=w_qkv, w_rate=w_rate, w_out=w_out, fw_gain=fw_gain, fast_first=fast_first, fast_third=fast_third, fast_second=fast_second)


coeff_a = 3.4445
coeff_b = -4.775
coeff_c = 2.0315
fast_step = 0.5
norm_eps = 1e-06

def inner_rows(left, right):
    return lax.dot_general(left, right, (((0,), (0,)), ((), ())), preferred_element_type=jnp.float32)

def silu_grad(hidden):
    sigma = jax.nn.sigmoid(hidden)
    return sigma * (1.0 + hidden * (1.0 - sigma))

def narrow(weights):
    return tuple((weight.astype(jnp.bfloat16) for weight in weights))

def fast_apply(queries, narrowed):
    hidden_one = jnp.dot(queries, narrowed[0], preferred_element_type=jnp.float32)
    hidden_three = jnp.dot(queries, narrowed[1], preferred_element_type=jnp.float32)
    activ = (jax.nn.silu(hidden_one) * hidden_three).astype(jnp.bfloat16)
    return jnp.dot(activ, narrowed[2], preferred_element_type=jnp.float32)

def fast_grads(keys, values, rates, narrowed):
    hidden_one = jnp.dot(keys, narrowed[0], preferred_element_type=jnp.float32)
    hidden_three = jnp.dot(keys, narrowed[1], preferred_element_type=jnp.float32)
    activ = (jax.nn.silu(hidden_one) * hidden_three).astype(jnp.bfloat16)
    target = (-rates[:, None] * values.astype(jnp.float32)).astype(jnp.bfloat16)
    grad_second = inner_rows(activ, target)
    dactiv = lax.dot_general(target, narrowed[2], (((1,), (1,)), ((), ())), preferred_element_type=jnp.float32)
    d_first = (dactiv * hidden_three * silu_grad(hidden_one)).astype(jnp.bfloat16)
    d_third = (dactiv * jax.nn.silu(hidden_one)).astype(jnp.bfloat16)
    return (inner_rows(keys, d_first), inner_rows(keys, d_third), grad_second)

def gram_of(current):
    return lax.dot_general(current, current, (((0,), (0,)), ((), ())), precision=lax.Precision.HIGHEST, preferred_element_type=jnp.float32)

def ns_update(current, gram):
    poly = coeff_b * gram + coeff_c * jnp.dot(gram, gram, precision=lax.Precision.HIGHEST)
    return coeff_a * current + jnp.dot(current, poly, precision=lax.Precision.HIGHEST)

def orthogonalize(grad):
    current = grad / jnp.sqrt(jnp.sum(grad * grad) + norm_eps)
    for step_num in range(NS_STEPS):
        current = ns_update(current, gram_of(current))
    return current

def window_softmax(query_rows, key_rows, value_rows, first_key):
    row_count = query_rows.shape[0]
    key_span = key_rows.shape[0]
    window_len = key_span - row_count
    scores = lax.dot_general(query_rows, key_rows, (((1,), (1,)), ((), ())), preferred_element_type=jnp.float32)
    scores = scores * query_rows.shape[1] ** (-0.5)
    offsets = window_len + lax.broadcasted_iota(jnp.int32, (row_count, key_span), 0) - lax.broadcasted_iota(jnp.int32, (row_count, key_span), 1)
    positions = first_key + lax.broadcasted_iota(jnp.int32, (row_count, key_span), 1)
    allowed = (offsets >= 0) & (offsets < window_len) & (positions >= 0)
    scores = jnp.where(allowed, scores, -1e+30)
    highest = lax.optimization_barrier(jnp.max(scores, axis=1, keepdims=True))
    weights = jnp.exp(scores - highest)
    weights = (weights / lax.optimization_barrier(jnp.sum(weights, axis=1, keepdims=True))).astype(jnp.bfloat16)
    return jnp.dot(weights, value_rows, preferred_element_type=jnp.float32)

def attend(queries, keys, values):
    total_rows = queries.shape[0]
    pad_keys = jnp.pad(keys, ((WINDOW, 0), (0, 0)))
    pad_values = jnp.pad(values, ((WINDOW, 0), (0, 0)))

    def one_block(block_num):
        start = (block_num * TOK_DEV).astype(jnp.int32)
        query_rows = lax.dynamic_slice_in_dim(queries, start, TOK_DEV, 0)
        key_rows = lax.dynamic_slice_in_dim(pad_keys, start, WINDOW + TOK_DEV, 0)
        value_rows = lax.dynamic_slice_in_dim(pad_values, start, WINDOW + TOK_DEV, 0)
        return window_softmax(query_rows, key_rows, value_rows, start - WINDOW)
    outputs = lax.map(one_block, jnp.arange(total_rows // TOK_DEV, dtype=jnp.int32))
    return outputs.reshape(total_rows, DH)

def reference(tokens, w_qkv, w_rate, w_out, fw_gain, fast_first, fast_third, fast_second):
    flat = tokens.reshape(BLOCKS * BLOCK, D)
    projected = jnp.dot(flat, w_qkv.reshape(D, HEADS * 3 * DH), preferred_element_type=jnp.float32).astype(jnp.bfloat16)
    projected = projected.reshape(BLOCKS * BLOCK, HEADS, 3, DH)
    rates = jax.nn.softplus(jnp.dot(flat, w_rate, preferred_element_type=jnp.float32))
    mixed = jnp.zeros((BLOCKS * BLOCK, D), jnp.float32)
    final_first = []
    final_third = []
    final_second = []
    for head_num in range(HEADS):
        queries = projected[:, head_num, 0]
        keys = projected[:, head_num, 1]
        values = projected[:, head_num, 2]
        attended = attend(queries, keys, values)
        current = (fast_first[head_num], fast_third[head_num], fast_second[head_num])
        outputs = []
        for block_num in range(BLOCKS):
            lower = block_num * BLOCK
            upper = lower + BLOCK
            outputs.append(fast_apply(queries[lower:upper], narrow(current)))
            if block_num + 1 < BLOCKS:
                grads = fast_grads(keys[lower:upper], values[lower:upper], rates[lower:upper, head_num], narrow(current))
                current = tuple((weight - fast_step * orthogonalize(grad) for weight, grad in zip(current, grads)))
        fast_out = jnp.concatenate(outputs, axis=0)
        normed = fast_out * lax.rsqrt(lax.optimization_barrier(jnp.mean(fast_out * fast_out, axis=1, keepdims=True)) + norm_eps) * fw_gain[head_num]
        combined = (attended + normed).astype(jnp.bfloat16)
        mixed = mixed + jnp.dot(combined, w_out[head_num], preferred_element_type=jnp.float32)
        final_first.append(current[0])
        final_third.append(current[1])
        final_second.append(current[2])
    mixed = mixed.astype(jnp.bfloat16).reshape(BLOCKS, BLOCK, D)
    return (mixed, jnp.stack(final_first), jnp.stack(final_third), jnp.stack(final_second))
```

```python
import functools

import jax
import jax.numpy as jnp
from jax import lax
from jax.experimental import pallas as pl
from jax.experimental.pallas import tpu as pltpu
from jax.sharding import PartitionSpec as P

WINDOW = 2048
NS_STEPS = 5

coeff_a = 3.4445
coeff_b = -4.775
coeff_c = 2.0315
fast_step = 0.5
norm_eps = 1e-06
BF = jnp.bfloat16
F32 = jnp.float32
VMEM = pl.BlockSpec(memory_space=pltpu.VMEM)
LIMIT = 60 * 1024 * 1024


def mm(left, right, dims):
    return lax.dot_general(left, right, (dims, ((), ())), preferred_element_type=F32)


def nn(left, right):
    return mm(left, right, ((1,), (0,)))


def nt(left, right):
    return mm(left, right, ((1,), (1,)))


def tn(left, right):
    return mm(left, right, ((0,), (0,)))


def project_kernel(rows, tok, w, wr, f1, f3, f2, q_ref, kv_ref, g_ref, kv_s):
    step = pl.program_id(0)
    res = nn(tok[...], w[...]).astype(BF)

    @pl.when(step < 2)
    def _():
        kv_ref[...] = res
        kv_s[step] = res

    @pl.when(step == 2)
    def _():
        q_ref[...] = res
        keys = kv_s[0, :rows]
        vals = kv_s[1, :rows]
        logit = jnp.sum(
            tok[:rows].astype(F32) * wr[...].astype(F32), axis=1, keepdims=True
        )
        rate = jnp.maximum(logit, 0.0) + jnp.log1p(jnp.exp(-jnp.abs(logit)))
        target = (-rate * vals.astype(F32)).astype(BF)
        h1 = nn(keys, f1[...].astype(BF))
        h3 = nn(keys, f3[...].astype(BF))
        sig = jax.nn.sigmoid(h1)
        silu = h1 * sig
        act = (silu * h3).astype(BF)
        dact = nt(target, f2[...].astype(BF))
        d1 = (dact * h3 * (sig * (1.0 + h1 * (1.0 - sig)))).astype(BF)
        d3 = (dact * silu).astype(BF)
        g_ref[0] = tn(keys, d1).astype(BF)
        g_ref[1] = tn(keys, d3).astype(BF)
        g_ref[2] = tn(act, target).astype(BF)


def project(flat, rows, w_qkv, w_rate, f1, f3, f2):
    total, width = flat.shape
    dh = f1.shape[0]
    fh = f1.shape[1]
    whole = lambda *shape: pl.BlockSpec(shape, lambda n: (0,) * len(shape))
    return pl.pallas_call(
        functools.partial(project_kernel, rows),
        grid=(3,),
        in_specs=[
            whole(total, width),
            pl.BlockSpec((width, dh), lambda n: (0, lax.rem(n + 1, 3))),
            whole(1, width),
            whole(dh, fh),
            whole(dh, fh),
            whole(fh, dh),
        ],
        out_specs=[
            whole(total, dh),
            pl.BlockSpec((total, dh), lambda n: (0, jnp.minimum(n, 1))),
            whole(3, dh, fh),
        ],
        out_shape=[
            jax.ShapeDtypeStruct((total, dh), BF),
            jax.ShapeDtypeStruct((total, 2 * dh), BF),
            jax.ShapeDtypeStruct((3, dh, fh), BF),
        ],
        scratch_shapes=[pltpu.VMEM((2, total, dh), BF)],
        compiler_params=pltpu.CompilerParams(vmem_limit_bytes=LIMIT),
        cost_estimate=pl.CostEstimate(
            flops=2 * total * width * 3 * dh, bytes_accessed=2 * width * 3 * dh, transcendentals=0
        ),
        name="project",
    )(flat, w_qkv, w_rate, f1, f3, f2)


def ns_kernel(g_ref, f1, f3, f2, o1, o3, o2, x_ref):
    for i in range(3):
        g = g_ref[i].astype(F32)
        x_ref[i] = g * lax.rsqrt(jnp.sum(g * g) + norm_eps)

    def step(_, carry):
        for i in range(3):
            x = x_ref[i]
            xb = x.astype(BF)
            gram = nt(xb, xb)
            gb = gram.astype(BF)
            poly = coeff_b * gram + coeff_c * nn(gb, gb)
            x_ref[i] = coeff_a * x + nn(poly.astype(BF), xb)
        return carry

    lax.fori_loop(0, NS_STEPS, step, 0)
    for i, (f, o) in enumerate(((f1, o1), (f3, o3), (f2, o2))):
        o[...] = f[...] - fast_step * x_ref[i]


def newton(total, f1, f3, f2):
    shape = f1.shape
    return pl.pallas_call(
        ns_kernel,
        in_specs=[VMEM] * 4,
        out_specs=[VMEM] * 3,
        out_shape=[jax.ShapeDtypeStruct(shape, F32)] * 3,
        scratch_shapes=[pltpu.VMEM((3,) + shape, F32)],
        compiler_params=pltpu.CompilerParams(vmem_limit_bytes=LIMIT // 2),
        cost_estimate=pl.CostEstimate(
            flops=45 * 2 * shape[0] ** 3, bytes_accessed=9 << 20, transcendentals=0
        ),
        name="newton",
    )(total, f1, f3, f2)


def attend_kernel(reach, blocks, n_ctx, q_ref, kv_ref, o_ref, m_s, l_s, acc):
    me = lax.axis_index("ctx")
    rows = q_ref.shape[0] // blocks
    dh = q_ref.shape[1]
    scale = dh ** (-0.5)
    for b in range(blocks):
        here = b * n_ctx + me
        q = q_ref[b * rows : (b + 1) * rows]
        m_s[...] = jnp.full_like(m_s, -1e30)
        l_s[...] = jnp.zeros_like(l_s)
        acc[...] = jnp.zeros_like(acc)

        def piece(s, carry):
            g = here - reach + s
            dev = lax.rem(g, n_ctx)
            at = pl.multiple_of(lax.div(g, n_ctx) * rows, rows)
            k = kv_ref[dev, pl.ds(at, rows), :dh]
            v = kv_ref[dev, pl.ds(at, rows), dh:]
            sc = nt(q, k) * scale
            diff = lax.broadcasted_iota(jnp.int32, (rows, rows), 0) - lax.broadcasted_iota(
                jnp.int32, (rows, rows), 1
            )
            off = diff + (reach - s) * rows
            sc = jnp.where((off >= 0) & (off < WINDOW), sc, -1e30)
            old = m_s[...]
            new = jnp.maximum(old, jnp.max(sc, axis=1, keepdims=True))
            p = jnp.where(sc > -1e29, jnp.exp(sc - new), 0.0)
            fade = jnp.exp(old - new)
            l_s[...] = l_s[...] * fade + jnp.sum(p, axis=1, keepdims=True)
            acc[...] = acc[...] * fade + nn(p.astype(BF), v)
            m_s[...] = new
            return carry

        lax.fori_loop(jnp.maximum(reach - here, 0), reach + 1, piece, 0)
        o_ref[b * rows : (b + 1) * rows] = acc[...] / l_s[...]


def attend(q, kv, blocks, n_ctx):
    rows = q.shape[0] // blocks
    dh = q.shape[1]
    reach = WINDOW // rows
    return pl.pallas_call(
        functools.partial(attend_kernel, reach, blocks, n_ctx),
        in_specs=[VMEM] * 2,
        out_specs=VMEM,
        out_shape=jax.ShapeDtypeStruct(q.shape, F32),
        scratch_shapes=[
            pltpu.VMEM((rows, 1), F32),
            pltpu.VMEM((rows, 1), F32),
            pltpu.VMEM((rows, dh), F32),
        ],
        compiler_params=pltpu.CompilerParams(vmem_limit_bytes=LIMIT),
        cost_estimate=pl.CostEstimate(
            flops=4 * q.shape[0] * dh * (WINDOW + rows),
            bytes_accessed=q.shape[0] * dh * 2 * 20,
            transcendentals=0,
        ),
        name="attend",
    )(q, kv)


def finish_kernel(q_ref, at_ref, f1, f3, f2, gain, wo, o_ref):
    q = q_ref[...]
    h1 = nn(q, f1[...].astype(BF))
    h3 = nn(q, f3[...].astype(BF))
    act = (jax.nn.silu(h1) * h3).astype(BF)
    out = nn(act, f2[...].astype(BF))
    inv = lax.rsqrt(jnp.mean(out * out, axis=1, keepdims=True) + norm_eps)
    both = (at_ref[...] + out * inv * gain[...]).astype(BF)
    o_ref[...] = nn(both, wo[...]).astype(BF)


def finish(q, att, f1, f3, f2, gain, wo):
    return pl.pallas_call(
        finish_kernel,
        in_specs=[VMEM] * 7,
        out_specs=VMEM,
        out_shape=jax.ShapeDtypeStruct((q.shape[0], wo.shape[1]), BF),
        compiler_params=pltpu.CompilerParams(vmem_limit_bytes=LIMIT // 2),
        cost_estimate=pl.CostEstimate(
            flops=2 * q.shape[0] * wo.shape[0] * (wo.shape[1] + 1536),
            bytes_accessed=6 << 20,
            transcendentals=0,
        ),
        name="finish",
    )(q, att, f1, f3, f2, gain, wo)


def shards(tokens, w_qkv, w_rate, w_out, fw_gain, fast_first, fast_third, fast_second):
    blocks, rows, width = tokens.shape
    dh = w_out.shape[1]
    n_ctx = lax.axis_size("ctx")
    flat = tokens.reshape(blocks * rows, width)
    fast = (fast_first[0], fast_third[0], fast_second[0])
    q, kv, grads = project(
        flat, rows, w_qkv.reshape(width, 3 * dh), w_rate.reshape(1, width), *fast
    )
    total = lax.psum(grads, "ctx")
    every = lax.all_gather(kv, "ctx")
    att = attend(q, every, blocks, n_ctx)
    current = fast
    mixed = []
    for b in range(blocks):
        part = slice(b * rows, (b + 1) * rows)
        terms = finish(q[part], att[part], *current, fw_gain, w_out[0])
        mixed.append(lax.psum_scatter(terms, "head", scatter_dimension=1, tiled=True))
        if b + 1 < blocks:
            current = newton(total, *current)
    return (jnp.stack(mixed),) + tuple(f[None] for f in current)


def solution(mesh):
    placed = (
        P(None, "ctx", None),
        P(None, "head", None),
        P(None, "head"),
        P("head", None, None),
        P("head", None),
        P("head", None, None),
        P("head", None, None),
        P("head", None, None),
    )
    return jax.shard_map(
        shards,
        mesh=mesh,
        in_specs=placed,
        out_specs=(
            P(None, "ctx", "head"),
            P("head", None, None),
            P("head", None, None),
            P("head", None, None),
        ),
        check_vma=False,
    )
```

```python
import functools

import jax
import jax.numpy as jnp
from jax import lax
from jax.experimental import pallas as pl
from jax.experimental.pallas import tpu as pltpu
from jax.sharding import PartitionSpec as P

WINDOW = 2048
NS_STEPS = 5

coeff_a = 3.4445
coeff_b = -4.775
coeff_c = 2.0315
fast_step = 0.5
norm_eps = 1e-06
BF = jnp.bfloat16
F32 = jnp.float32
VMEM = pl.BlockSpec(memory_space=pltpu.VMEM)
LIMIT = 60 * 1024 * 1024


def mm(left, right, dims):
    return lax.dot_general(left, right, (dims, ((), ())), preferred_element_type=F32)


def nn(left, right):
    return mm(left, right, ((1,), (0,)))


def nt(left, right):
    return mm(left, right, ((1,), (1,)))


def tn(left, right):
    return mm(left, right, ((0,), (0,)))


def project_kernel(rows, tok, w, wr, f1, f3, f2, q_ref, kv_ref, g_ref, kv_s):
    step = pl.program_id(0)
    res = nn(tok[...], w[...]).astype(BF)

    @pl.when(step < 2)
    def _():
        kv_ref[...] = res
        kv_s[step] = res

    @pl.when(step == 2)
    def _():
        q_ref[...] = res
        keys = kv_s[0, :rows]
        vals = kv_s[1, :rows]
        logit = jnp.sum(
            tok[:rows].astype(F32) * wr[...].astype(F32), axis=1, keepdims=True
        )
        rate = jnp.maximum(logit, 0.0) + jnp.log1p(jnp.exp(-jnp.abs(logit)))
        target = (-rate * vals.astype(F32)).astype(BF)
        h1 = nn(keys, f1[...].astype(BF))
        h3 = nn(keys, f3[...].astype(BF))
        sig = jax.nn.sigmoid(h1)
        silu = h1 * sig
        act = (silu * h3).astype(BF)
        dact = nt(target, f2[...].astype(BF))
        d1 = (dact * h3 * (sig * (1.0 + h1 * (1.0 - sig)))).astype(BF)
        d3 = (dact * silu).astype(BF)
        g_ref[0] = tn(keys, d1).astype(BF)
        g_ref[1] = tn(keys, d3).astype(BF)
        g_ref[2] = tn(act, target).astype(BF)


def project(flat, rows, w_qkv, w_rate, f1, f3, f2):
    total, width = flat.shape
    dh = f1.shape[0]
    fh = f1.shape[1]
    whole = lambda *shape: pl.BlockSpec(shape, lambda n: (0,) * len(shape))
    return pl.pallas_call(
        functools.partial(project_kernel, rows),
        grid=(3,),
        in_specs=[
            whole(total, width),
            pl.BlockSpec((width, dh), lambda n: (0, lax.rem(n + 1, 3))),
            whole(1, width),
            whole(dh, fh),
            whole(dh, fh),
            whole(fh, dh),
        ],
        out_specs=[
            whole(total, dh),
            pl.BlockSpec((total, dh), lambda n: (0, jnp.minimum(n, 1))),
            whole(3, dh, fh),
        ],
        out_shape=[
            jax.ShapeDtypeStruct((total, dh), BF),
            jax.ShapeDtypeStruct((total, 2 * dh), BF),
            jax.ShapeDtypeStruct((3, dh, fh), BF),
        ],
        scratch_shapes=[pltpu.VMEM((2, total, dh), BF)],
        compiler_params=pltpu.CompilerParams(vmem_limit_bytes=LIMIT),
        cost_estimate=pl.CostEstimate(
            flops=2 * total * width * 3 * dh, bytes_accessed=2 * width * 3 * dh, transcendentals=0
        ),
        name="project",
    )(flat, w_qkv, w_rate, f1, f3, f2)


def cross_bits(n, sub):
    bits = [1 << i for i in range(1, n.bit_length() - 1)]
    return bits if sub == 0 else bits[::-1]


def remote(src, dst, send, recv, axis, peer):
    return pltpu.make_async_remote_copy(
        src_ref=src,
        dst_ref=dst,
        send_sem=send,
        recv_sem=recv,
        device_id={axis: peer},
        device_id_type=pl.DeviceIdType.MESH,
    )


def mix_kernel(
    n, nh, blocks, q_ref, kv_ref, g_ref, f1, f3, f2, gain, wo,
    mixed, o1, o3, o2,
    every, half_in, sums, sum_in, total, m_s, l_s, acc, t_buf, t_in,
    h_send, h_recv, d_send, d_recv, a_send, a_recv, k_send, k_recv, r_send, r_recv,
):
    me = lax.axis_index("ctx")
    hme = lax.axis_index("head")
    rows = q_ref.shape[0] // blocks
    dh = q_ref.shape[1]
    reach = WINDOW // rows
    scale = dh ** (-0.5)
    cols = wo.shape[1] // nh
    half = g_ref.shape[1] // 2
    quarter = half // 2
    piece_rows = rows // 2
    core = lax.rem(me, 2)
    mine = pl.multiple_of(core * half, half)
    theirs = pl.multiple_of((1 - core) * half, half)
    levels = n.bit_length() - 2

    barrier = pltpu.get_barrier_semaphore()
    ctx_bits = [1 << i for i in range(n.bit_length() - 1)]
    for bit in ctx_bits:
        pl.semaphore_signal(
            barrier, inc=1, device_id={"ctx": me ^ bit}, device_id_type=pl.DeviceIdType.MESH
        )
    for r in range(1, nh):
        pl.semaphore_signal(
            barrier,
            inc=1,
            device_id={"head": lax.rem(hme + r, nh)},
            device_id_type=pl.DeviceIdType.MESH,
        )
    pl.semaphore_wait(barrier, len(ctx_bits) + nh - 1)

    started = []

    def go(copy):
        copy.start()
        started.append(copy)

    def place(p):
        return pl.ds((p // 2) * rows + (p % 2) * piece_rows, piece_rows)

    def kv_copy(p, c, bit):
        dst = every.at[me ^ c, place(p)]
        src = kv_ref.at[place(p)] if c == 0 else dst
        return remote(
            src, dst, k_send.at[p, c | bit], k_recv.at[p, c | bit], "ctx", me ^ bit
        )

    def kv_wait(p, c):
        dst = every.at[me ^ c, place(p)]
        bit = c & -c
        remote(dst, dst, k_send.at[p, c], k_recv.at[p, c], "ctx", me ^ bit).wait_recv()

    def later(p, c):
        order = cross_bits(n, p % 2)
        last = max([i for i, bit in enumerate(order) if c & bit], default=-1)
        return order[last + 1 :]

    def pass_on(p, c):
        for bit in later(p, c):
            go(kv_copy(p, c, bit))
        go(kv_copy(p, c, 1))

    def first_hop(p):
        return cross_bits(n, p % 2)[0]

    def part(u):
        return pl.ds(u * quarter, quarter)

    def sum_copy(t, u):
        return remote(
            sums.at[t, :, part(u)],
            sum_in.at[t, :, part(u)],
            a_send.at[t, u],
            a_recv.at[t, u],
            "ctx",
            me ^ cross_bits(n, u)[t],
        )

    first = remote(g_ref.at[:, pl.ds(theirs, half)], half_in, h_send, h_recv, "ctx", me ^ 1)
    go(first)
    every[me] = kv_ref[...]
    first.wait_recv()
    sums[0] = (g_ref[:, pl.ds(mine, half)].astype(F32) + half_in[...].astype(F32)).astype(BF)
    for t in range(levels):
        step = [sum_copy(t, u) for u in range(2)]
        for copy in step:
            go(copy)
        if t == levels - 1:
            for p in range(2):
                for bit in cross_bits(n, p):
                    go(kv_copy(p, 0, bit))
            for p in range(2 * blocks):
                go(kv_copy(p, 0, 1))
        for copy in step:
            copy.wait_recv()
        added = (sums[t].astype(F32) + sum_in[t].astype(F32)).astype(BF)
        if t < levels - 1:
            sums[t + 1] = added
        else:
            total[:, pl.ds(mine, half)] = added
    done = total.at[:, pl.ds(mine, half)]
    give = remote(done, done, d_send, d_recv, "ctx", me ^ 1)
    go(give)
    other = total.at[:, pl.ds(theirs, half)]
    remote(other, other, d_send, d_recv, "ctx", me ^ 1).wait_recv()

    for i, x_ref in enumerate((o1, o3, o2)):
        g = total[i].astype(F32)
        x_ref[...] = g * lax.rsqrt(jnp.sum(g * g) + norm_eps)

    def ns_step(_, carry):
        for x_ref in (o1, o3, o2):
            x = x_ref[...]
            xb = x.astype(BF)
            gram = nt(xb, xb)
            gb = gram.astype(BF)
            poly = coeff_b * gram + coeff_c * nn(gb, gb)
            x_ref[...] = coeff_a * x + nn(poly.astype(BF), xb)
        return carry

    early = 3
    lax.fori_loop(0, early, ns_step, 0)
    for p in range(2):
        kv_wait(p, first_hop(p))
        pass_on(p, first_hop(p))
    for p in range(2, 2 * blocks):
        for bit in cross_bits(n, p % 2):
            go(kv_copy(p, 0, bit))
    lax.fori_loop(early, NS_STEPS, ns_step, 0)
    for f, o in ((f1, o1), (f3, o3), (f2, o2)):
        o[...] = f[...] - fast_step * o[...]

    def gather_rest(b):
        pieces = (2 * b, 2 * b + 1)
        evens = sorted(range(2, n, 2), key=lambda c: (bin(c).count("1"), c))
        for c in evens:
            for p in pieces:
                if c != first_hop(p):
                    kv_wait(p, c)
                    pass_on(p, c)
        for c in range(1, n, 2):
            for p in pieces:
                kv_wait(p, c)

    def clear():
        m_s[...] = jnp.full_like(m_s, -1e30)
        l_s[...] = jnp.zeros_like(l_s)
        acc[...] = jnp.zeros_like(acc)

    def attend(b, side):
        here = b * n + me
        q = q_ref[b * rows : (b + 1) * rows]

        def piece(g, carry):
            dev = g - side * n
            k = every[dev, side * rows : (side + 1) * rows, :dh]
            v = every[dev, side * rows : (side + 1) * rows, dh:]
            sc = nt(q, k) * scale
            diff = lax.broadcasted_iota(jnp.int32, (rows, rows), 0) - lax.broadcasted_iota(
                jnp.int32, (rows, rows), 1
            )
            off = diff + (here - g) * rows
            sc = jnp.where((off >= 0) & (off < WINDOW), sc, -1e30)
            old = m_s[...]
            new = jnp.maximum(old, jnp.max(sc, axis=1, keepdims=True))
            p = jnp.where(sc > -1e29, jnp.exp(sc - new), 0.0)
            fade = jnp.exp(old - new)
            l_s[...] = l_s[...] * fade + jnp.sum(p, axis=1, keepdims=True)
            acc[...] = acc[...] * fade + nn(p.astype(BF), v)
            m_s[...] = new
            return carry

        low = jnp.maximum(here - reach, side * n)
        high = jnp.minimum(here, side * n + n - 1)
        lax.fori_loop(low, high + 1, piece, 0)

    def head_copy(b, r):
        peer = lax.rem(hme + r, nh)
        return remote(
            t_buf.at[b, peer],
            t_in.at[b, r - 1],
            r_send.at[b, r - 1],
            r_recv.at[b, r - 1],
            "head",
            peer,
        )

    def finish(b, w1, w3, w2):
        q = q_ref[b * rows : (b + 1) * rows]
        h1 = nn(q, w1[...].astype(BF))
        h3 = nn(q, w3[...].astype(BF))
        act = (jax.nn.silu(h1) * h3).astype(BF)
        out = nn(act, w2[...].astype(BF))
        inv = lax.rsqrt(jnp.mean(out * out, axis=1, keepdims=True) + norm_eps)
        both = (acc[...] / l_s[...] + out * inv * gain[...]).astype(BF)
        for h in range(nh):
            t_buf[b, h] = nn(both, wo[:, h * cols : (h + 1) * cols]).astype(BF)
        copies = [head_copy(b, r) for r in range(1, nh)]
        for copy in copies:
            go(copy)
        return copies

    head_copies = []
    for b in range(blocks):
        clear()
        if b > 0:
            for p in (2 * b, 2 * b + 1):
                kv_wait(p, first_hop(p))
                pass_on(p, first_hop(p))
            attend(b, b - 1)
        gather_rest(b)
        attend(b, b)
        head_copies.append(finish(b, *((f1, f3, f2) if b == 0 else (o1, o3, o2))))
    for b in range(blocks):
        for copy in head_copies[b]:
            copy.wait_recv()
        result = t_buf[b, hme].astype(F32)
        for r in range(nh - 1):
            result = result + t_in[b, r].astype(F32)
        mixed[b] = result.astype(BF)
    for copy in started:
        copy.wait_send()


def mix(n, nh, blocks, q, kv, grads, f1, f3, f2, gain, wo):
    rows = q.shape[0] // blocks
    dh, fh = f1.shape
    cols = wo.shape[1] // nh
    levels = n.bit_length() - 2
    dma = pltpu.SemaphoreType.DMA
    return pl.pallas_call(
        functools.partial(mix_kernel, n, nh, blocks),
        in_specs=[VMEM] * 8,
        out_specs=[VMEM] * 4,
        out_shape=[jax.ShapeDtypeStruct((blocks, rows, cols), BF)]
        + [jax.ShapeDtypeStruct(f.shape, F32) for f in (f1, f3, f2)],
        scratch_shapes=[
            pltpu.VMEM((n,) + kv.shape, BF),
            pltpu.VMEM((3, dh // 2, fh), BF),
            pltpu.VMEM((levels, 3, dh // 2, fh), BF),
            pltpu.VMEM((levels, 3, dh // 2, fh), BF),
            pltpu.VMEM((3, dh, fh), BF),
            pltpu.VMEM((rows, 1), F32),
            pltpu.VMEM((rows, 1), F32),
            pltpu.VMEM((rows, dh), F32),
            pltpu.VMEM((blocks, nh, rows, cols), BF),
            pltpu.VMEM((blocks, nh - 1, rows, cols), BF),
            dma,
            dma,
            dma,
            dma,
            dma((levels, 2)),
            dma((levels, 2)),
            dma((2 * blocks, n)),
            dma((2 * blocks, n)),
            dma((blocks, nh - 1)),
            dma((blocks, nh - 1)),
        ],
        compiler_params=pltpu.CompilerParams(
            vmem_limit_bytes=63 * 1024 * 1024, collective_id=0, has_side_effects=True
        ),
        name="mix",
    )(q, kv, grads, f1, f3, f2, gain, wo)


def shards(tokens, w_qkv, w_rate, w_out, fw_gain, fast_first, fast_third, fast_second):
    blocks, rows, width = tokens.shape
    dh = w_out.shape[1]
    n_ctx = lax.axis_size("ctx")
    flat = tokens.reshape(blocks * rows, width)
    fast = (fast_first[0], fast_third[0], fast_second[0])
    q, kv, grads = project(
        flat, rows, w_qkv.reshape(width, 3 * dh), w_rate.reshape(1, width), *fast
    )
    mixed, *current = mix(
        n_ctx, lax.axis_size("head"), blocks, q, kv, grads, *fast, fw_gain, w_out[0]
    )
    return (mixed,) + tuple(f[None] for f in current)


def solution(mesh):
    placed = (
        P(None, "ctx", None),
        P(None, "head", None),
        P(None, "head"),
        P("head", None, None),
        P("head", None),
        P("head", None, None),
        P("head", None, None),
        P("head", None, None),
    )
    return jax.shard_map(
        shards,
        mesh=mesh,
        in_specs=placed,
        out_specs=(
            P(None, "ctx", "head"),
            P("head", None, None),
            P("head", None, None),
            P("head", None, None),
        ),
        check_vma=False,
    )
```

```python
import functools

import jax
import jax.numpy as jnp
from jax import lax
from jax.experimental import pallas as pl
from jax.experimental.pallas import tpu as pltpu
from jax.sharding import PartitionSpec as P

WINDOW = 2048
NS_STEPS = 5

coeff_a = 3.4445
coeff_b = -4.775
coeff_c = 2.0315
fast_step = 0.5
norm_eps = 1e-06
BF = jnp.bfloat16
F32 = jnp.float32
VMEM = pl.BlockSpec(memory_space=pltpu.VMEM)
LIMIT = 60 * 1024 * 1024


def mm(left, right, dims):
    return lax.dot_general(left, right, (dims, ((), ())), preferred_element_type=F32)


def nn(left, right):
    return mm(left, right, ((1,), (0,)))


def nt(left, right):
    return mm(left, right, ((1,), (1,)))


def tn(left, right):
    return mm(left, right, ((0,), (0,)))


def project_kernel(rows, tok, w, wr, f1, f3, f2, q_ref, kv_ref, g_ref, kv_s):
    step = pl.program_id(0)
    res = nn(tok[...], w[...]).astype(BF)

    @pl.when(step < 2)
    def _():
        kv_ref[...] = res
        kv_s[step] = res

    @pl.when(step == 2)
    def _():
        q_ref[...] = res
        keys = kv_s[0, :rows]
        vals = kv_s[1, :rows]
        logit = jnp.sum(
            tok[:rows].astype(F32) * wr[...].astype(F32), axis=1, keepdims=True
        )
        rate = jnp.maximum(logit, 0.0) + jnp.log1p(jnp.exp(-jnp.abs(logit)))
        target = (-rate * vals.astype(F32)).astype(BF)
        h1 = nn(keys, f1[...].astype(BF))
        h3 = nn(keys, f3[...].astype(BF))
        sig = jax.nn.sigmoid(h1)
        silu = h1 * sig
        act = (silu * h3).astype(BF)
        dact = nt(target, f2[...].astype(BF))
        d1 = (dact * h3 * (sig * (1.0 + h1 * (1.0 - sig)))).astype(BF)
        d3 = (dact * silu).astype(BF)
        g_ref[0] = tn(keys, d1).astype(BF)
        g_ref[1] = tn(keys, d3).astype(BF)
        g_ref[2] = tn(act, target).astype(BF)


def project(flat, rows, w_qkv, w_rate, f1, f3, f2):
    total, width = flat.shape
    dh = f1.shape[0]
    fh = f1.shape[1]
    whole = lambda *shape: pl.BlockSpec(shape, lambda n: (0,) * len(shape))
    return pl.pallas_call(
        functools.partial(project_kernel, rows),
        grid=(3,),
        in_specs=[
            whole(total, width),
            pl.BlockSpec((width, dh), lambda n: (0, lax.rem(n + 1, 3))),
            whole(1, width),
            whole(dh, fh),
            whole(dh, fh),
            whole(fh, dh),
        ],
        out_specs=[
            whole(total, dh),
            pl.BlockSpec((total, dh), lambda n: (0, jnp.minimum(n, 1))),
            whole(3, dh, fh),
        ],
        out_shape=[
            jax.ShapeDtypeStruct((total, dh), BF),
            jax.ShapeDtypeStruct((total, 2 * dh), BF),
            jax.ShapeDtypeStruct((3, dh, fh), BF),
        ],
        scratch_shapes=[pltpu.VMEM((2, total, dh), BF)],
        compiler_params=pltpu.CompilerParams(vmem_limit_bytes=LIMIT),
        cost_estimate=pl.CostEstimate(
            flops=2 * total * width * 3 * dh, bytes_accessed=2 * width * 3 * dh, transcendentals=0
        ),
        name="project",
    )(flat, w_qkv, w_rate, f1, f3, f2)


def cross_bits(n, sub):
    bits = [1 << i for i in range(1, n.bit_length() - 1)]
    return bits if sub == 0 else bits[::-1]


def remote(src, dst, send, recv, axis, peer):
    return pltpu.make_async_remote_copy(
        src_ref=src,
        dst_ref=dst,
        send_sem=send,
        recv_sem=recv,
        device_id={axis: peer},
        device_id_type=pl.DeviceIdType.MESH,
    )


def mix_kernel(
    n, nh, blocks, q_ref, kv_ref, g_ref, f1, f3, f2, gain, wo,
    mixed, o1, o3, o2,
    every, half_in, sums, sum_in, total, m_s, l_s, acc, t_buf, t_in,
    h_send, h_recv, d_send, d_recv, a_send, a_recv, k_send, k_recv, r_send, r_recv,
):
    me = lax.axis_index("ctx")
    hme = lax.axis_index("head")
    rows = q_ref.shape[0] // blocks
    dh = q_ref.shape[1]
    reach = WINDOW // rows
    scale = dh ** (-0.5)
    cols = wo.shape[1] // nh
    half = g_ref.shape[1] // 2
    quarter = half // 2
    piece_rows = rows // 2
    core = lax.rem(me, 2)
    mine = pl.multiple_of(core * half, half)
    theirs = pl.multiple_of((1 - core) * half, half)
    levels = n.bit_length() - 2

    barrier = pltpu.get_barrier_semaphore()
    ctx_bits = [1 << i for i in range(n.bit_length() - 1)]
    for bit in ctx_bits:
        pl.semaphore_signal(
            barrier, inc=1, device_id={"ctx": me ^ bit}, device_id_type=pl.DeviceIdType.MESH
        )
    for r in range(1, nh):
        pl.semaphore_signal(
            barrier,
            inc=1,
            device_id={"head": lax.rem(hme + r, nh)},
            device_id_type=pl.DeviceIdType.MESH,
        )
    pl.semaphore_wait(barrier, len(ctx_bits) + nh - 1)

    started = []

    def go(copy):
        copy.start()
        started.append(copy)

    def place(p):
        return pl.ds((p // 2) * rows + (p % 2) * piece_rows, piece_rows)

    def kv_copy(p, c, bit):
        dst = every.at[me ^ c, place(p)]
        src = kv_ref.at[place(p)] if c == 0 else dst
        return remote(
            src, dst, k_send.at[p, c | bit], k_recv.at[p, c | bit], "ctx", me ^ bit
        )

    def kv_wait(p, c):
        dst = every.at[me ^ c, place(p)]
        bit = c & -c
        remote(dst, dst, k_send.at[p, c], k_recv.at[p, c], "ctx", me ^ bit).wait_recv()

    def later(p, c):
        order = cross_bits(n, p % 2)
        last = max([i for i, bit in enumerate(order) if c & bit], default=-1)
        return order[last + 1 :]

    def pass_on(p, c):
        for bit in later(p, c):
            go(kv_copy(p, c, bit))
        go(kv_copy(p, c, 1))

    def first_hop(p):
        return cross_bits(n, p % 2)[0]

    def part(u):
        return pl.ds(u * quarter, quarter)

    def sum_copy(t, u):
        return remote(
            sums.at[t, :, part(u)],
            sum_in.at[t, :, part(u)],
            a_send.at[t, u],
            a_recv.at[t, u],
            "ctx",
            me ^ cross_bits(n, u)[t],
        )

    first = remote(g_ref.at[:, pl.ds(theirs, half)], half_in, h_send, h_recv, "ctx", me ^ 1)
    go(first)
    every[me] = kv_ref[...]
    first.wait_recv()
    sums[0] = (g_ref[:, pl.ds(mine, half)].astype(F32) + half_in[...].astype(F32)).astype(BF)
    for t in range(levels):
        step = [sum_copy(t, u) for u in range(2)]
        for copy in step:
            go(copy)
        if t == levels - 1:
            for p in range(2):
                for bit in cross_bits(n, p):
                    go(kv_copy(p, 0, bit))
            for p in range(2 * blocks):
                go(kv_copy(p, 0, 1))
        for copy in step:
            copy.wait_recv()
        added = (sums[t].astype(F32) + sum_in[t].astype(F32)).astype(BF)
        if t < levels - 1:
            sums[t + 1] = added
        else:
            total[:, pl.ds(mine, half)] = added
    done = total.at[:, pl.ds(mine, half)]
    give = remote(done, done, d_send, d_recv, "ctx", me ^ 1)
    go(give)
    other = total.at[:, pl.ds(theirs, half)]
    remote(other, other, d_send, d_recv, "ctx", me ^ 1).wait_recv()

    for i, x_ref in enumerate((o1, o3, o2)):
        g = total[i].astype(F32)
        x_ref[...] = g * lax.rsqrt(jnp.sum(g * g) + norm_eps)

    def ns_step(_, carry):
        for x_ref in (o1, o3, o2):
            x = x_ref[...]
            xb = x.astype(BF)
            gram = nt(xb, xb)
            gb = gram.astype(BF)
            poly = coeff_b * gram + coeff_c * nn(gb, gb)
            x_ref[...] = coeff_a * x + nn(poly.astype(BF), xb)
        return carry

    early = 3
    lax.fori_loop(0, early, ns_step, 0)
    for p in range(2):
        kv_wait(p, first_hop(p))
        pass_on(p, first_hop(p))
    for p in range(2, 2 * blocks):
        for bit in cross_bits(n, p % 2):
            go(kv_copy(p, 0, bit))
    lax.fori_loop(early, NS_STEPS, ns_step, 0)
    for f, o in ((f1, o1), (f3, o3), (f2, o2)):
        o[...] = f[...] - fast_step * o[...]

    def gather_attend(b):
        pieces = (2 * b, 2 * b + 1)
        here = b * n + me
        evens = range(0, n, 2)
        for count in range(n.bit_length() - 1):
            group = [c for c in evens if bin(c).count("1") == count]
            for c in group:
                for p in pieces:
                    if c and c != first_hop(p):
                        kv_wait(p, c)
                        pass_on(p, c)
            for c in group:
                for p in pieces:
                    kv_wait(p, c | 1)
                for one in (c, c | 1):
                    g = b * n + (me ^ one)

                    @pl.when((g <= here) & (g >= here - reach))
                    def _():
                        attend(b, b, g)

    def clear():
        m_s[...] = jnp.full_like(m_s, -1e30)
        l_s[...] = jnp.zeros_like(l_s)
        acc[...] = jnp.zeros_like(acc)

    def attend(b, side, only=None):
        here = b * n + me
        q = q_ref[b * rows : (b + 1) * rows]

        def piece(g, carry):
            dev = g - side * n
            k = every[dev, side * rows : (side + 1) * rows, :dh]
            v = every[dev, side * rows : (side + 1) * rows, dh:]
            sc = nt(q, k) * scale
            diff = lax.broadcasted_iota(jnp.int32, (rows, rows), 0) - lax.broadcasted_iota(
                jnp.int32, (rows, rows), 1
            )
            off = diff + (here - g) * rows
            sc = jnp.where((off >= 0) & (off < WINDOW), sc, -1e30)
            old = m_s[...]
            new = jnp.maximum(old, jnp.max(sc, axis=1, keepdims=True))
            p = jnp.where(sc > -1e29, jnp.exp(sc - new), 0.0)
            fade = jnp.exp(old - new)
            l_s[...] = l_s[...] * fade + jnp.sum(p, axis=1, keepdims=True)
            acc[...] = acc[...] * fade + nn(p.astype(BF), v)
            m_s[...] = new
            return carry

        if only is not None:
            piece(only, 0)
            return
        low = jnp.maximum(here - reach, side * n)
        high = jnp.minimum(here, side * n + n - 1)
        lax.fori_loop(low, high + 1, piece, 0)

    def head_copy(b, r):
        peer = lax.rem(hme + r, nh)
        return remote(
            t_buf.at[b, peer],
            t_in.at[b, r - 1],
            r_send.at[b, r - 1],
            r_recv.at[b, r - 1],
            "head",
            peer,
        )

    def finish(b, w1, w3, w2):
        q = q_ref[b * rows : (b + 1) * rows]
        h1 = nn(q, w1[...].astype(BF))
        h3 = nn(q, w3[...].astype(BF))
        act = (jax.nn.silu(h1) * h3).astype(BF)
        out = nn(act, w2[...].astype(BF))
        inv = lax.rsqrt(jnp.mean(out * out, axis=1, keepdims=True) + norm_eps)
        both = (acc[...] / l_s[...] + out * inv * gain[...]).astype(BF)
        for h in range(nh):
            t_buf[b, h] = nn(both, wo[:, h * cols : (h + 1) * cols]).astype(BF)
        copies = [head_copy(b, r) for r in range(1, nh)]
        for copy in copies:
            go(copy)
        return copies

    head_copies = []
    for b in range(blocks):
        clear()
        if b > 0:
            for p in (2 * b, 2 * b + 1):
                kv_wait(p, first_hop(p))
                pass_on(p, first_hop(p))
            attend(b, b - 1)
        gather_attend(b)
        head_copies.append(finish(b, *((f1, f3, f2) if b == 0 else (o1, o3, o2))))
    for b in range(blocks):
        for copy in head_copies[b]:
            copy.wait_recv()
        result = t_buf[b, hme].astype(F32)
        for r in range(nh - 1):
            result = result + t_in[b, r].astype(F32)
        mixed[b] = result.astype(BF)
    for copy in started:
        copy.wait_send()


def mix(n, nh, blocks, q, kv, grads, f1, f3, f2, gain, wo):
    rows = q.shape[0] // blocks
    dh, fh = f1.shape
    cols = wo.shape[1] // nh
    levels = n.bit_length() - 2
    dma = pltpu.SemaphoreType.DMA
    return pl.pallas_call(
        functools.partial(mix_kernel, n, nh, blocks),
        in_specs=[VMEM] * 8,
        out_specs=[VMEM] * 4,
        out_shape=[jax.ShapeDtypeStruct((blocks, rows, cols), BF)]
        + [jax.ShapeDtypeStruct(f.shape, F32) for f in (f1, f3, f2)],
        scratch_shapes=[
            pltpu.VMEM((n,) + kv.shape, BF),
            pltpu.VMEM((3, dh // 2, fh), BF),
            pltpu.VMEM((levels, 3, dh // 2, fh), BF),
            pltpu.VMEM((levels, 3, dh // 2, fh), BF),
            pltpu.VMEM((3, dh, fh), BF),
            pltpu.VMEM((rows, 1), F32),
            pltpu.VMEM((rows, 1), F32),
            pltpu.VMEM((rows, dh), F32),
            pltpu.VMEM((blocks, nh, rows, cols), BF),
            pltpu.VMEM((blocks, nh - 1, rows, cols), BF),
            dma,
            dma,
            dma,
            dma,
            dma((levels, 2)),
            dma((levels, 2)),
            dma((2 * blocks, n)),
            dma((2 * blocks, n)),
            dma((blocks, nh - 1)),
            dma((blocks, nh - 1)),
        ],
        compiler_params=pltpu.CompilerParams(
            vmem_limit_bytes=63 * 1024 * 1024, collective_id=0, has_side_effects=True
        ),
        name="mix",
    )(q, kv, grads, f1, f3, f2, gain, wo)


def shards(tokens, w_qkv, w_rate, w_out, fw_gain, fast_first, fast_third, fast_second):
    blocks, rows, width = tokens.shape
    dh = w_out.shape[1]
    n_ctx = lax.axis_size("ctx")
    flat = tokens.reshape(blocks * rows, width)
    fast = (fast_first[0], fast_third[0], fast_second[0])
    q, kv, grads = project(
        flat, rows, w_qkv.reshape(width, 3 * dh), w_rate.reshape(1, width), *fast
    )
    mixed, *current = mix(
        n_ctx, lax.axis_size("head"), blocks, q, kv, grads, *fast, fw_gain, w_out[0]
    )
    return (mixed,) + tuple(f[None] for f in current)


def solution(mesh):
    placed = (
        P(None, "ctx", None),
        P(None, "head", None),
        P(None, "head"),
        P("head", None, None),
        P("head", None),
        P("head", None, None),
        P("head", None, None),
        P("head", None, None),
    )
    return jax.shard_map(
        shards,
        mesh=mesh,
        in_specs=placed,
        out_specs=(
            P(None, "ctx", "head"),
            P("head", None, None),
            P("head", None, None),
            P("head", None, None),
        ),
        check_vma=False,
    )
```
